512 devices in a mesh: frame: 64 (over y, z_lo, core), state: 8 (over z_hi, x).
Axes of the slice: x: 4, y: 4, z: 16 (z_hi: 2, z_lo: 8; z = z_hi * 8 + z_lo), core: 2. Of those that a mesh axis runs over, the one named last changes fastest.
Arguments:
- object_slices: float32 [2, 2, 16384, 512], P(None, None, 'frame'), may hold values from -4 to 4
- probe: float32 [8, 2, 256, 256], P('state'), may hold values from -4 to 4
- amplitude: float32 [64, 256, 256], P('frame'), may hold values from 0.5 to 4
- positions: int32 [64, 2], P('frame'), may hold values from 0 to 256, as said below
- propagator: float32 [256, 256], replicated, may hold values from -3.140625 to 3.140625
Outputs:
- gradient: float32 [2, 2, 16384, 512], P(None, None, ('frame', 'state'))
The draws below stay inside these ranges and needn't reach their ends.
Inputs may be any that keep to these rules, and one draw needn't show every extreme that they name: positions[f, 0] is the row offset of frame f's patch within the rows owned by its owner f, from 0 to 255; positions[f, 1] is its column offset, from 0 to 256.
All inputs are finite; a program needn't handle non-finite values.
Results may differ from the reference program's by a relative error of at most 0.0001.
Values sent between devices are 32-bit elements; how exact they have to be, the bound alone decides.
A program may use at most 64 MiB of HBM per device.

```python
import math
import jax
import jax.numpy as jnp
from jax import lax

P_SIZE = 256
F_DEV = 1
TILE = 256
OBJ_COLS = 512
STATES = 8
FRAMES = 64
OBJ_ROWS = 16384


def draw_positions(key, part):
    row_key = jax.random.fold_in(key, 11)
    col_key = jax.random.fold_in(key, 23)
    rows_drawn = jax.random.randint(row_key, (FRAMES, 1), 0, TILE, dtype=jnp.int32)
    cols_drawn = jax.random.randint(col_key, (FRAMES, 1), 0, OBJ_COLS - P_SIZE + 1, dtype=jnp.int32)
    return jnp.concatenate([rows_drawn, cols_drawn], axis=1)


def shard_levels(stream_key, dims, shards, low, top_value):
    gain = 1.0
    for dim, blocks in shards:
        draws = jax.random.uniform(jax.random.fold_in(jax.random.fold_in(stream_key, 6), dim), (blocks,), jnp.float32, low / len(shards), top_value / len(shards))
        gain = gain * jnp.repeat(jnp.exp(draws), dims[dim] // blocks).reshape((-1,) + (1,) * (len(dims) - 1 - dim))
    return gain


def normal_values(stream_key, extent, spread, reach, shards=(), held_as=jnp.bfloat16):
    result = jax.random.normal(stream_key, extent, jnp.float32) * spread
    if len(shards) > 0:
        result = shard_levels(stream_key, extent, shards, -0.22, 0.18) * result
    return jnp.clip(result, min=-reach, max=reach).astype(held_as)


def setup_inputs(seed: int = 0) -> dict:
    key_of = jax.random.split(jax.random.key(seed), 6)
    return {
        "object_slices": normal_values(key_of[0], (2, 2, OBJ_ROWS, OBJ_COLS), 0.7, 4.0, ((2, 64),), jnp.float32),
        "probe": normal_values(key_of[1], (STATES, 2, P_SIZE, P_SIZE), 0.5, 4.0, ((0, 8),), jnp.float32),
        "amplitude": jnp.clip(jnp.exp(math.log(4.0) - 2.0794415 * jax.random.uniform(key_of[2], (FRAMES, P_SIZE, P_SIZE), jnp.float32) ** shard_levels(key_of[2], (FRAMES, P_SIZE, P_SIZE), ((0, 64),), -0.2, 0.2)), 0.5, 4.0),
        "positions": draw_positions(jax.random.fold_in(key_of[5], 71), 0),
        "propagator": jnp.clip(jax.random.uniform(key_of[4], (P_SIZE, P_SIZE), jnp.float32, -3.140625, 3.140625), -3.140625, 3.140625),
    }


def reference(object_slices, probe, amplitude, positions, propagator):
    rows_all = object_slices.shape[2]
    pixels = amplitude.shape[1]
    padded = jnp.concatenate([object_slices, object_slices[:, :, :pixels]], axis=2)
    field = padded[:, 0] + 1j * padded[:, 1]
    kernel = jnp.cos(propagator) + 1j * jnp.sin(propagator)
    modes = probe[:, 0] + 1j * probe[:, 1]
    owners = jnp.arange(FRAMES, dtype=jnp.int32) // F_DEV * TILE
    row_starts = (owners + positions[:, 0]).astype(jnp.int32)
    col_starts = positions[:, 1].astype(jnp.int32)

    def forward(values):
        return jnp.fft.fft2(values, axes=(-2, -1), norm='ortho')

    def inverse(values):
        return jnp.fft.ifft2(values, axes=(-2, -1), norm='ortho')

    def step(summed, inputs):
        row_at, col_at, measured = inputs
        zero_at = jnp.zeros((), jnp.int32)
        corner = (zero_at, row_at, col_at)
        patch = lax.dynamic_slice(field, corner, (2, pixels, pixels))
        wave = modes * patch[0]
        inner = inverse(kernel * forward(wave))
        far = forward(patch[1] * inner)
        intensity = lax.optimization_barrier(jnp.sum(jnp.real(far) ** 2 + jnp.imag(far) ** 2, axis=0))
        factor = 1.0 - measured / jnp.sqrt(intensity + 1.0)
        back = inverse(factor * far)
        second = lax.optimization_barrier(jnp.sum(jnp.conj(inner) * back, axis=0))
        chi = jnp.conj(patch[1]) * back
        front = inverse(jnp.conj(kernel) * forward(chi))
        first = lax.optimization_barrier(jnp.sum(jnp.conj(modes) * front, axis=0))
        present = lax.dynamic_slice(summed, corner, (2, pixels, pixels))
        summed = lax.dynamic_update_slice(summed, present + jnp.stack([first, second]), corner)
        return (summed, None)
    start = jnp.zeros(field.shape, field.dtype)
    summed, unused = lax.scan(step, start, (row_starts, col_starts, amplitude))
    folded = summed[:, :rows_all]
    folded = folded.at[:, :pixels].add(summed[:, rows_all:])
    return jnp.stack([jnp.real(folded), jnp.imag(folded)], axis=1)
```

```python
import jax
import jax.numpy as jnp
import numpy as np
from jax import lax
from jax.experimental import pallas as pl
from jax.experimental.pallas import tpu as pltpu
from jax.sharding import PartitionSpec as P

MESH = pl.DeviceIdType.MESH
F32 = jnp.float32
BF16 = jnp.bfloat16
N = 256
H = N // 2

POS, PZ, PY, PD, HALO, INT, FAC, GR, GRB, RET, NSEM = 0, 1, 2, 5, 6, 8, 11, 14, 20, 26, 28


def real_form(m):
    return np.block([[m.real, -m.imag], [m.imag, m.real]])


def split_tables():
    k = np.arange(H)
    even = np.exp(-2j * np.pi * ((np.outer(k, k) * 2) % N) / N) / 16.0
    odd = np.exp(-2j * np.pi * ((np.outer(2 * k + 1, k)) % N) / N) / 16.0
    mats = [real_form(even), real_form(odd)]
    mats += [m.T.copy() for m in mats]
    out = []
    for m in mats:
        m = m.astype(np.float32)
        hi = m.astype(BF16)
        lo = (m - hi.astype(np.float32)).astype(BF16)
        out.append(np.stack([hi, lo]))
    return np.stack(out)


def cat(parts, axis):
    return jnp.concatenate(parts, axis=axis)


def dot(a, b):
    return jnp.dot(a, b, preferred_element_type=F32)


def halves(v):
    hi = v.astype(BF16)
    lo = (v - hi.astype(F32)).astype(BF16)
    return hi, lo


def thirds(v):
    hi = v.astype(BF16)
    rest = v - hi.astype(F32)
    mid = rest.astype(BF16)
    lo = (rest - mid.astype(F32)).astype(BF16)
    return hi, mid, lo


def pick_rows(sel, v):
    hi, mid, lo = thirds(v)
    return dot(sel, hi) + dot(sel, mid) + dot(sel, lo)


def pick_cols(v, sel):
    hi, mid, lo = thirds(v)
    return dot(hi, sel) + dot(mid, sel) + dot(lo, sel)


def one_hot(cond):
    return jnp.where(cond, 1.0, 0.0).astype(F32).astype(BF16)


def iota(shape, dim):
    return lax.broadcasted_iota(jnp.int32, shape, dim)


def freq(i):
    return jnp.where(i < H, 2 * i, 2 * i - (N - 1))


def kernel(
    pos_s, obj_h, probe_h, amp_h, prop_h, tab_h, out_ref,
    obj, probe, amp, prop, rt, lt, pos, posn, hs, hr, pb,
    pr, ker, ampb, patch, inner, far, work, sl, sr, isend, irecv, fac, g, gr, grb, rets, retr,
    lsem, tsem, ssem, rsem,
):
    f = lax.axis_index("frame")
    s = lax.axis_index("state")
    x = s % 4
    zh = s // 4
    core = f % 2
    y = f // 16
    edge = f % 16 == 15
    fn = (f + 1) % 64
    fp = (f + 63) % 64
    flip = (s + 4) % 8
    nxt = (fn, jnp.where(edge, flip, s))
    prv = (fp, jnp.where(f % 16 == 0, flip, s))
    zl = (f // 2) % 8
    zdev = (jnp.where(zl >= 4, f - 8, f + 8), flip)
    other = (jnp.where(core == 0, f + 1, f - 1), s)
    ydev = [((f + 16 * k) % 64, s) for k in (1, 2, 3)]
    xid = [(x + k) % 4 for k in (1, 2, 3)]
    xdev = [(f, zh * 4 + i) for i in xid]
    part = core * 4 + y

    local = [
        pltpu.make_async_copy(probe_h.at[0], probe, lsem.at[0]),
        pltpu.make_async_copy(obj_h, obj, lsem.at[1]),
        pltpu.make_async_copy(prop_h, prop, lsem.at[2]),
        pltpu.make_async_copy(amp_h.at[0], amp, lsem.at[3]),
    ]
    for c in local:
        c.start()
    tables = []
    for i in range(4):
        for j, hl in enumerate((0, 0, 1)):
            tables.append((tab_h.at[(i + 2) % 4, hl], rt.at[i, pl.ds(N * j, N), :]))
        for j, hl in enumerate((0, 1, 0)):
            tables.append((tab_h.at[i, hl], lt.at[i, :, pl.ds(N * j, N)]))
    tables = [pltpu.make_async_copy(a, b, tsem.at[i]) for i, (a, b) in enumerate(tables)]
    for c in tables:
        c.start()

    row = pos_s[0, 0]
    col = pos_s[0, 1]
    pos[0] = jnp.full((8, N), row, jnp.int32)
    pos[1] = jnp.full((8, N), col, jnp.int32)

    peers = [nxt, prv, zdev, other, *ydev, *xdev]
    barrier = pltpu.get_barrier_semaphore()
    for d in peers:
        pl.semaphore_signal(barrier, inc=1, device_id=d, device_id_type=MESH)
    pl.semaphore_wait(barrier, len(peers))

    def remote(src, dst, slot, dev):
        return pltpu.make_async_remote_copy(
            src_ref=src, dst_ref=dst, send_sem=ssem.at[slot], recv_sem=rsem.at[slot],
            device_id=dev, device_id_type=MESH,
        )

    started = []

    def send(*args):
        c = remote(*args)
        c.start()
        started.append(c)
        return c

    c_pos = send(pos, posn, POS, nxt)
    local[0].wait()
    c_pz = send(probe.at[:, pl.ds(pl.multiple_of(part * 32, 32), 32), :], pb.at[part], PZ, zdev)
    local[1].wait()

    c_pos.wait_recv()
    lanes = iota((N, N), 1)
    rows = iota((N, N), 0)
    colp = posn[1, 0:1, :]
    keep = lanes >= colp
    c_halo = []
    for i in range(2):
        for p in range(2):
            hs[i, p] = jnp.where(keep, obj[i, p, :, 0:N], obj[i, p, :, N : 2 * N])
        c_halo.append(send(hs.at[i], hr.at[i], HALO + i, prv))

    zcol = one_hot(rows == freq(lanes))
    zrow = one_hot(lanes == freq(rows))
    local[2].wait()
    phase = pick_cols(pick_rows(zrow, prop[...]), zcol)
    ker[0] = jnp.cos(phase)
    ker[1] = jnp.sin(phase)
    local[3].wait()
    zown = one_hot(iota((64, N), 1) == freq(iota((64, N), 0) + 64 * x))
    ampb[...] = pick_cols(pick_rows(zown, amp[...]), zcol)

    turn_r = one_hot(((rows - lanes - row) & (N - 1)) == 0)
    turn_c = one_hot(((lanes - rows - col) & (N - 1)) == 0)
    for p in range(2):
        pr[0, p] = pick_cols(pick_rows(turn_r, probe[p]), turn_c)
    for c in tables:
        c.wait()

    def stage_l(st, i, v):
        hi, lo = halves(v)
        sl[st, i, 0:N, :] = hi
        sl[st, i, N : 2 * N, :] = hi
        sl[st, i, 2 * N : 3 * N, :] = lo

    def stage_r(st, i, v):
        hi, lo = halves(v)
        sr[st, i, :, 0:N] = hi
        sr[st, i, :, N : 2 * N] = lo
        sr[st, i, :, 2 * N : 3 * N] = hi

    def left_fwd(st, re, im):
        stage_l(st, 0, cat([re[:H] + re[H:], im[:H] + im[H:]], 0))
        stage_l(st, 1, cat([re[:H] - re[H:], im[:H] - im[H:]], 0))
        e = dot(lt[0], sl[st, 0])
        o = dot(lt[1], sl[st, 1])
        return cat([e[:H], o[:H]], 0), cat([e[H:], o[H:]], 0)

    def right_fwd(st, re, im):
        stage_r(st, 0, cat([re[:, :H] + re[:, H:], im[:, :H] + im[:, H:]], 1))
        stage_r(st, 1, cat([re[:, :H] - re[:, H:], im[:, :H] - im[:, H:]], 1))
        e = dot(sr[st, 0], rt[0])
        o = dot(sr[st, 1], rt[1])
        return cat([e[:, :H], o[:, :H]], 1), cat([e[:, H:], o[:, H:]], 1)

    def right_inv(st, re, im):
        stage_r(st, 0, cat([re[:, :H], im[:, :H]], 1))
        stage_r(st, 1, cat([re[:, H:], im[:, H:]], 1))
        a = dot(sr[st, 0], rt[2])
        b = dot(sr[st, 1], rt[3])
        u, v = a + b, a - b
        return cat([u[:, :H], v[:, :H]], 1), cat([u[:, H:], v[:, H:]], 1)

    def left_inv(st, re, im):
        stage_l(st, 0, cat([re[:H], im[:H]], 0))
        stage_l(st, 1, cat([re[H:], im[H:]], 0))
        a = dot(lt[2], sl[st, 0])
        b = dot(lt[3], sl[st, 1])
        u, v = a + b, a - b
        return cat([u[:H], v[:H]], 0), cat([u[H:], v[H:]], 0)

    def through(st, fun, re, im):
        re, im = fun(st, re, im)
        work[st, 0] = re
        work[st, 1] = im

    def dft(st, re, im):
        through(st, left_fwd, re, im)
        through(st, right_fwd, work[st, 0], work[st, 1])

    def idft(st, re, im):
        through(st, right_inv, re, im)
        through(st, left_inv, work[st, 0], work[st, 1])

    own_row = rows >= row
    own_left = lanes >= col

    def fill_patch(i):
        for p in range(2):
            own = jnp.where(own_left, obj[i, p, :, 0:N], obj[i, p, :, N : 2 * N])
            patch[i, p] = jnp.where(own_row, own, hr[i, p])

    def forward_inner(st):
        a, b = pr[st, 0], pr[st, 1]
        u, v = patch[0, 0], patch[0, 1]
        dft(st, a * u - b * v, a * v + b * u)
        a, b = ker[0], ker[1]
        u, v = work[st, 0], work[st, 1]
        idft(st, a * u - b * v, a * v + b * u)
        inner[st, 0] = work[st, 0]
        inner[st, 1] = work[st, 1]

    def forward_far(st):
        a, b = patch[1, 0], patch[1, 1]
        u, v = inner[st, 0], inner[st, 1]
        dft(st, a * u - b * v, a * v + b * u)
        far[st, 0] = work[st, 0]
        far[st, 1] = work[st, 1]

    c_pz.wait_recv()
    c_py = [send(pb.at[part], pb.at[part], PY + k, ydev[k]) for k in range(3)]
    c_halo[0].wait_recv()
    fill_patch(0)
    forward_inner(0)
    for c in c_py:
        c.wait_recv()
    slab = pb.at[pl.ds(core * 4, 4)]
    c_pd = send(slab, slab, PD, other)
    c_pd.wait_recv()
    for p in range(2):
        pr[1, p] = pick_cols(pick_rows(turn_r, pb[:, p].reshape(N, N)), turn_c)
    forward_inner(1)
    c_halo[1].wait_recv()
    fill_patch(1)
    forward_far(0)
    forward_far(1)

    isend[...] = (
        far[0, 0] * far[0, 0] + far[0, 1] * far[0, 1] + far[1, 0] * far[1, 0] + far[1, 1] * far[1, 1]
    )
    c_int = [
        send(isend.at[pl.ds(pl.multiple_of(xid[k] * 64, 64), 64), :], irecv.at[k], INT + k, xdev[k])
        for k in range(3)
    ]
    mine = pl.ds(pl.multiple_of(x * 64, 64), 64)
    total = isend[mine, :]
    for k in range(3):
        c_int[k].wait_recv()
        total = total + irecv[k]
    fac[mine, :] = 1.0 - ampb[...] / jnp.sqrt(total + 1.0)
    c_fac = [send(fac.at[mine, :], fac.at[mine, :], FAC + k, xdev[k]) for k in range(3)]
    for k in range(3):
        c_fac[k].wait_recv()

    for st in range(2):
        idft(st, fac[...] * far[st, 0], fac[...] * far[st, 1])
        a, b = inner[st, 0], inner[st, 1]
        u, v = work[st, 0], work[st, 1]
        re, im = a * u + b * v, a * v - b * u
        if st == 0:
            g[1, 0] = re
            g[1, 1] = im
        else:
            g[1, 0] += re
            g[1, 1] += im

    def shares(i, half, to, base):
        return [
            remote(
                g.at[i, :, pl.ds(pl.multiple_of(half * H + xid[k] * 32, 32), 32), :],
                to.at[i, k], base + 3 * i + k, xdev[k],
            )
            for k in range(3)
        ]

    def send_shares(i):
        for c in shares(i, zh, gr, GR):
            c.start()

        @pl.when(edge)
        def _():
            for c in shares(i, 1 - zh, grb, GRB):
                c.start()

    first = pl.multiple_of(zh * H + x * 32, 32)

    def collect(i):
        for c in shares(i, zh, gr, GR):
            c.wait_recv()
        for p in range(2):
            own = g[i, p, pl.ds(first, 32), :]
            for k in range(3):
                own = own + gr[i, k, p]
            rets[i, p] = own
            out_ref[i, p, :, 0:N] = jnp.where(mask_l, own, 0.0)
            out_ref[i, p, :, N : 2 * N] = jnp.where(mask_r, own, 0.0)

        @pl.when(edge)
        def _():
            there = pl.multiple_of((1 - zh) * H + x * 32, 32)
            for c in shares(i, 1 - zh, grb, GRB):
                c.wait_recv()
            for p in range(2):
                own = g[i, p, pl.ds(there, 32), :]
                for k in range(3):
                    own = own + grb[i, k, p]
                rets[i, p] = own

        return send(rets.at[i], retr.at[i], RET + i, nxt)

    q = iota((32, N), 0) + first
    pcol = iota((32, N), 1)
    mask_l = (q >= row) & (pcol >= col)
    mask_r = (q >= row) & (pcol < col)
    prow = q < posn[0, 0:1, :]
    pl_l = prow & (pcol >= posn[1, 0:1, :])
    pl_r = prow & (pcol < posn[1, 0:1, :])

    def deliver(i, c):
        c.wait_recv()
        for p in range(2):
            got = retr[i, p]
            out_ref[i, p, :, 0:N] += jnp.where(pl_l, got, 0.0)
            out_ref[i, p, :, N : 2 * N] += jnp.where(pl_r, got, 0.0)

    send_shares(1)
    for st in range(2):
        a, b = patch[1, 0], patch[1, 1]
        u, v = work[st, 0], work[st, 1]
        dft(st, a * u + b * v, a * v - b * u)
        a, b = ker[0], ker[1]
        u, v = work[st, 0], work[st, 1]
        idft(st, a * u + b * v, a * v - b * u)
        a, b = pr[st, 0], pr[st, 1]
        u, v = work[st, 0], work[st, 1]
        re, im = a * u + b * v, a * v - b * u
        if st == 0:
            g[0, 0] = re
            g[0, 1] = im
        else:
            g[0, 0] += re
            g[0, 1] += im
    send_shares(0)
    c_ret1 = collect(1)
    c_ret0 = collect(0)
    deliver(1, c_ret1)
    deliver(0, c_ret0)

    for c in started:
        c.wait_send()
    for i in range(2):
        for c in shares(i, zh, gr, GR):
            c.wait_send()

    @pl.when(edge)
    def _():
        for i in range(2):
            for c in shares(i, 1 - zh, grb, GRB):
                c.wait_send()


def on_device(object_slices, probe, amplitude, positions, propagator):
    any_spec = pl.BlockSpec(memory_space=pl.ANY)
    vm = pltpu.VMEM
    return pl.pallas_call(
        kernel,
        name="ptycho",
        out_shape=jax.ShapeDtypeStruct((2, 2, 32, 2 * N), F32),
        in_specs=[pl.BlockSpec(memory_space=pltpu.SMEM)] + [any_spec] * 5,
        out_specs=pl.BlockSpec(memory_space=pltpu.VMEM),
        scratch_shapes=[
            vm((2, 2, N, 2 * N), F32),
            vm((2, N, N), F32),
            vm((N, N), F32),
            vm((N, N), F32),
            vm((4, 3 * N, N), BF16),
            vm((4, N, 3 * N), BF16),
            vm((2, 8, N), jnp.int32),
            vm((2, 8, N), jnp.int32),
            vm((2, 2, N, N), F32),
            vm((2, 2, N, N), F32),
            vm((8, 2, 32, N), F32),
            vm((2, 2, N, N), F32),
            vm((2, N, N), F32),
            vm((64, N), F32),
            vm((2, 2, N, N), F32),
            vm((2, 2, N, N), F32),
            vm((2, 2, N, N), F32),
            vm((2, 2, N, N), F32),
            vm((2, 2, 3 * N, N), BF16),
            vm((2, 2, N, 3 * N), BF16),
            vm((N, N), F32),
            vm((3, 64, N), F32),
            vm((N, N), F32),
            vm((2, 2, N, N), F32),
            vm((2, 3, 2, 32, N), F32),
            vm((2, 3, 2, 32, N), F32),
            vm((2, 2, 32, N), F32),
            vm((2, 2, 32, N), F32),
            pltpu.SemaphoreType.DMA((4,)),
            pltpu.SemaphoreType.DMA((24,)),
            pltpu.SemaphoreType.DMA((NSEM,)),
            pltpu.SemaphoreType.DMA((NSEM,)),
        ],
        compiler_params=pltpu.CompilerParams(collective_id=0, has_side_effects=True),
    )(positions, object_slices, probe, amplitude, propagator, jnp.asarray(split_tables()))


def solution(mesh):
    in_specs = (
        P(None, None, "frame", None),
        P("state", None, None, None),
        P("frame", None, None),
        P("frame", None),
        P(),
    )
    out_specs = P(None, None, ("frame", "state"), None)
    return jax.shard_map(
        on_device, mesh=mesh, in_specs=in_specs, out_specs=out_specs, check_vma=False
    )
```
